32 devices in a mesh: rep: 4 (over x, core), fsdp: 8 (over z, y).
Axes of the slice: x: 2, y: 2, z: 4, core: 2. Of those that a mesh axis runs over, the one named last changes fastest.
Arguments:
- layer_inputs: bfloat16 [8192, 4608], P(('rep', 'fsdp')), may hold values from -12 to 12
- queries: bfloat16 [8192, 2048], P(('rep', 'fsdp')), may hold values from -32 to 32
- saved_keys: bfloat16 [8192, 1024], P(('rep', 'fsdp')), may hold values from -6 to 6
- saved_values: bfloat16 [8192, 1024], P(('rep', 'fsdp')), may hold values from -6 to 6
- out_grad: bfloat16 [8192, 2048], P(('rep', 'fsdp')), may hold values from -0.625 to 0.625
- global_params: float32 [4608, 1024], P('fsdp'), may hold values from -0.09375 to 0.09375
- replica_params: float32 [4, 4608, 1024], P('rep', 'fsdp'), may hold values from -0.09375 to 0.09375
- outer_momentum: float32 [4608, 1024], P('fsdp'), may hold values from -0.125 to 0.125
- next_inputs: bfloat16 [8192, 4608], P(('rep', 'fsdp')), may hold values from -6 to 6
Outputs:
- new_params: float32 [4608, 1024], P('fsdp')
- new_momentum: float32 [4608, 1024], P('fsdp')
- next_keys: bfloat16 [8192, 1024], P(('rep', 'fsdp'))
The draws below stay inside these ranges and needn't reach their ends.
All inputs are finite; a program needn't handle non-finite values.
Results may differ from the reference program's by a relative error of at most 0.014.
Values may be sent and summed in bfloat16 or wider, within the bound.
A program may use at most 128 MiB of HBM per device.

```python
import jax
import jax.numpy as jnp
from jax import lax

D = 4608
QH = 16
KVH = 8
HD = 128
SEQ_LEN = 256
TOKENS = 8192
N_REP = 4
N_FSDP = 8


def spiked(array, stream_key, source, target, blocks, factor):
    owner, partner = [(jnp.arange(array.shape[position]) // (array.shape[position] // blocks)).reshape([-1 if axis == position else 1 for axis in range(array.ndim)]) for position in (source, target)]
    chosen = jax.random.permutation(stream_key, blocks)[partner]
    strong = (owner == chosen) | (owner == (partner + blocks // 2) % blocks)
    return jnp.where(strong, factor * array, array)


def shard_levels(rng, dims, shards, low, top_value):
    def one(position, parts):
        heights = jax.random.uniform(jax.random.fold_in(jax.random.fold_in(rng, 6), position), (parts,), jnp.float32, low / len(shards), top_value / len(shards))
        return jnp.repeat(jnp.exp(heights), dims[position] // parts).reshape((-1,) + (1,) * (len(dims) - position - 1))

    factor_of = one(*shards[0])
    for cut in shards[1:]:
        factor_of = factor_of * one(*cut)
    return factor_of


def centred(stream_key, shape, width, reach, cuts=(), dtype=jnp.bfloat16):
    loudness = shard_levels(stream_key, shape, cuts, -0.22, 0.18) if cuts else 1.0
    drawn = jax.random.normal(stream_key, shape, jnp.float32) * width * loudness
    return jnp.minimum(jnp.maximum(drawn, -reach), reach).astype(dtype)


def gaussian_with(rng, extent, deviation, reach, cuts, heavy, kind=jnp.bfloat16):
    drawn = deviation * jax.random.normal(rng, extent, jnp.float32)
    if cuts:
        drawn = drawn * shard_levels(rng, extent, cuts, -0.22, 0.18)
    return jnp.clip(spiked(drawn, jax.random.fold_in(rng, 3), *heavy), -reach, reach).astype(kind)


def setup_inputs(seed: int = 0) -> dict:
    streams_of = jax.random.split(jax.random.key(seed), 10)
    return {
        "layer_inputs": gaussian_with(streams_of[0], (TOKENS, D), 1.0, 12.0, ((0, 32),), (0, 1, 32, 2.75)),
        "queries": centred(streams_of[1], (TOKENS, QH * HD), 5.0, 32.0, ((0, 32),)),
        "saved_keys": centred(streams_of[2], (TOKENS, KVH * HD), 1.0, 6.0, ((0, 32),)),
        "saved_values": centred(streams_of[3], (TOKENS, KVH * HD), 1.0, 6.0, ((0, 32),)),
        "out_grad": centred(streams_of[4], (TOKENS, QH * HD), 0.1, 0.625, ((0, 32),)),
        "global_params": centred(streams_of[5], (D, KVH * HD), D ** -0.5, 0.09375, ((0, 8),), jnp.float32),
        "replica_params": centred(streams_of[6], (N_REP, D, KVH * HD), D ** -0.5, 0.09375, ((0, 4), (1, 8)), jnp.float32),
        "outer_momentum": centred(streams_of[7], (D, KVH * HD), 0.02, 0.125, ((0, 8),), jnp.float32),
        "next_inputs": centred(streams_of[8], (TOKENS, D), 1.0, 6.0, ((0, 32),)),
    }


score_scale = 1.0 / 12.0
soft_cap = 50.0
rope_base = 10000.0
inner_rate = 0.02
outer_rate = 0.7
outer_beta = 0.9


def rotate_back(grads, length):
    half = grads.shape[-1] // 2
    places = jnp.arange(length).astype(jnp.float32)
    freqs = rope_base ** (-jnp.arange(half).astype(jnp.float32) / half)
    angles = (places[:, None] * freqs[None, :])[:, None, :]
    cosine = jnp.cos(angles)
    sine = jnp.sin(angles)
    first = grads[..., :half]
    second = grads[..., half:]
    return jnp.concatenate([first * cosine + second * sine, second * cosine - first * sine], axis=-1)


def attention_keys(query_rows, key_rows, value_rows, grad_rows):
    length = query_rows.shape[0]
    group = QH // KVH
    query_wide = query_rows.astype(jnp.float32).reshape(length, KVH, group, HD)
    key_wide = key_rows.astype(jnp.float32).reshape(length, KVH, HD)
    value_wide = value_rows.astype(jnp.float32).reshape(length, KVH, HD)
    grad_wide = grad_rows.astype(jnp.float32).reshape(length, KVH, group, HD)
    logits = jnp.einsum("ihgd,jhd->hgij", query_wide, key_wide) * score_scale
    capped = jnp.tanh(logits / soft_cap)
    row_index = jnp.arange(length)
    causal = row_index[:, None] >= row_index[None, :]
    unnormed = jnp.where(causal, jnp.exp(soft_cap * capped), jnp.float32(0.0))
    probs = unnormed / jnp.sum(unnormed, axis=-1, keepdims=True)
    dprobs = jnp.einsum("ihgd,jhd->hgij", grad_wide, value_wide)
    center = jnp.sum(probs * dprobs, axis=-1, keepdims=True)
    dlogits = (probs * (dprobs - center) * (1.0 - capped * capped) * score_scale).astype(jnp.bfloat16)
    rotated = jnp.einsum("hgij,ihgd->jhd", dlogits.astype(jnp.float32), query_wide)
    plain = rotate_back(rotated, length)
    return plain.reshape(length, KVH * HD).astype(jnp.bfloat16)


def reference(layer_inputs, queries, saved_keys, saved_values, out_grad, global_params, replica_params, outer_momentum, next_inputs):
    seqs = N_REP * N_FSDP
    packed = (queries.reshape(seqs, SEQ_LEN, QH * HD), saved_keys.reshape(seqs, SEQ_LEN, KVH * HD),
              saved_values.reshape(seqs, SEQ_LEN, KVH * HD), out_grad.reshape(seqs, SEQ_LEN, QH * HD))
    key_grads = lax.map(lambda member: attention_keys(member[0], member[1], member[2], member[3]), packed)
    key_grads = key_grads.reshape(seqs * SEQ_LEN, KVH * HD)
    group_tokens = N_FSDP * SEQ_LEN
    summed = jnp.zeros(global_params.shape, jnp.float32)
    for replica in range(N_REP):
        token_rows = layer_inputs[replica * group_tokens:(replica + 1) * group_tokens]
        grad_rows = key_grads[replica * group_tokens:(replica + 1) * group_tokens]
        group_grad = jnp.dot(token_rows.T, grad_rows, preferred_element_type=jnp.float32)
        finished = replica_params[replica] - inner_rate * group_grad
        summed = summed + (global_params - finished)
    outer_grad = summed / N_REP
    new_momentum = outer_beta * outer_momentum + outer_grad
    new_params = global_params - outer_rate * (outer_grad + outer_beta * new_momentum)
    next_keys = jnp.dot(next_inputs, new_params.astype(jnp.bfloat16), preferred_element_type=jnp.float32).astype(jnp.bfloat16)
    return new_params, new_momentum, next_keys
```

```python
import functools

import jax
import jax.numpy as jnp
from jax import lax
from jax.experimental import pallas as pl
from jax.experimental.pallas import tpu as pltpu
from jax.sharding import PartitionSpec as P

QH = 16
KVH = 8
HD = 128


score_scale = 1.0 / 12.0
soft_cap = 50.0
rope_base = 10000.0
inner_rate = 0.02
outer_rate = 0.7
outer_beta = 0.9

MESH = pl.DeviceIdType.MESH


def rotate_back(grads, length):
    half = grads.shape[-1] // 2
    places = jnp.arange(length).astype(jnp.float32)
    freqs = rope_base ** (-jnp.arange(half).astype(jnp.float32) / half)
    angles = (places[:, None] * freqs[None, :])[:, None, :]
    cosine = jnp.cos(angles)
    sine = jnp.sin(angles)
    first = grads[..., :half]
    second = grads[..., half:]
    return jnp.concatenate(
        [first * cosine + second * sine, second * cosine - first * sine], axis=-1
    )


def attention_keys(query_rows, key_rows, value_rows, grad_rows):
    length = query_rows.shape[0]
    group = QH // KVH
    query_wide = query_rows.reshape(length, KVH, group, HD)
    key_wide = key_rows.reshape(length, KVH, HD)
    value_wide = value_rows.reshape(length, KVH, HD)
    grad_wide = grad_rows.reshape(length, KVH, group, HD)
    logits = (
        jnp.einsum("ihgd,jhd->hgij", query_wide, key_wide, preferred_element_type=jnp.float32)
        * score_scale
    )
    capped = jnp.tanh(logits / soft_cap)
    row_index = jnp.arange(length)
    causal = row_index[:, None] >= row_index[None, :]
    unnormed = jnp.where(causal, jnp.exp(soft_cap * capped), jnp.float32(0.0))
    probs = unnormed / jnp.sum(unnormed, axis=-1, keepdims=True)
    dprobs = jnp.einsum("ihgd,jhd->hgij", grad_wide, value_wide, preferred_element_type=jnp.float32)
    center = jnp.sum(probs * dprobs, axis=-1, keepdims=True)
    dlogits = (probs * (dprobs - center) * (1.0 - capped * capped) * score_scale).astype(
        jnp.bfloat16
    )
    rotated = jnp.einsum("hgij,ihgd->jhd", dlogits, query_wide, preferred_element_type=jnp.float32)
    plain = rotate_back(rotated, length)
    return plain.reshape(length, KVH * HD).astype(jnp.bfloat16)


def outer_kernel(
    part, glob, mom, weights, fresh, rc, r1a, r1b, r2a, r2b, s3, r3, send_sem, recv_sem
):
    lines, _, rows, cols = part.shape
    half, quarter, eighth = cols // 2, cols // 4, cols // 8
    rep, fsdp = lax.axis_index("rep"), lax.axis_index("fsdp")
    core, x = lax.rem(rep, 2), rep // 2
    y, z = lax.rem(fsdp, 2), fsdp // 2
    over_core = {"rep": rep + 1 - 2 * core}
    over_x = {"rep": rep + 2 - 4 * x}
    over_y = {"fsdp": fsdp + 1 - 2 * y}

    def over_z(line):
        return {"fsdp": line * 2 + y}

    def at(start, size):
        return pl.ds(pl.multiple_of(start, size), size)

    f32 = jnp.float32
    peers = [over_core, over_x, over_y] + [
        over_z(lax.rem(z + t, lines)) for t in range(1, lines)
    ]
    barrier = pltpu.get_barrier_semaphore()
    for peer in peers:
        pl.semaphore_signal(barrier, inc=1, device_id=peer, device_id_type=MESH)
    pl.semaphore_wait(barrier, len(peers))

    copies = {}

    def send(kind, step, src, dst, peer):
        slot = len(copies)
        copy = pltpu.make_async_remote_copy(
            src_ref=src,
            dst_ref=dst,
            send_sem=send_sem.at[slot],
            recv_sem=recv_sem.at[slot],
            device_id=peer,
            device_id_type=MESH,
        )
        copy.start()
        copies[kind, step] = copy

    def arrive(kind, step):
        copies[kind, step].wait_recv()

    def line_of(step):
        return lax.rem(z + 1 + step, lines)

    for s in range(lines):
        g = line_of(s)
        send("c", s, part.at[g, :, :, at((1 - core) * half, half)], rc.at[g], over_core)

    def sum_core(s):
        g = line_of(s)
        arrive("c", s)
        for yy in range(2):
            mine = part[g, yy, :, at(core * half, half)]
            rc[g, yy] = (rc[g, yy].astype(f32) + mine.astype(f32)).astype(rc.dtype)
        send("1a", s, rc.at[g, :, :, at((1 - x) * eighth, eighth)], r1a.at[g], over_x)
        send("1b", s, rc.at[g, 1 - y, :, quarter:half], r1b.at[g], over_y)

    def sum_first(s):
        g = line_of(s)
        arrive("1a", s)
        for yy in range(2):
            mine = rc[g, yy, :, at(x * eighth, eighth)]
            r1a[g, yy] = (r1a[g, yy].astype(f32) + mine.astype(f32)).astype(rc.dtype)
        send("2a", s, r1a.at[g, 1 - y], r2a.at[g], over_y)
        arrive("1b", s)
        mine = rc[g, y, :, quarter:half]
        r1b[g] = (r1b[g].astype(f32) + mine.astype(f32)).astype(rc.dtype)
        send("2b", s, r1b.at[g, :, at((1 - x) * eighth, eighth)], r2b.at[g], over_x)

    def sum_second(s):
        g = line_of(s)
        arrive("2a", s)
        sum_a = r2a[g].astype(f32) + r1a[g, y].astype(f32)
        arrive("2b", s)
        sum_b = r2b[g].astype(f32) + r1b[g, :, at(x * eighth, eighth)].astype(f32)
        if s == lines - 1:
            return sum_a, sum_b
        s3[s, :, :eighth] = sum_a.astype(s3.dtype)
        s3[s, :, eighth:] = sum_b.astype(s3.dtype)
        send("3", s, s3.at[s], r3.at[s], over_z(g))

    for tick in range(lines + 2):
        if 0 <= tick - 2:
            own = sum_second(tick - 2)
        if 0 <= tick - 1 < lines:
            sum_first(tick - 1)
        if tick < lines:
            sum_core(tick)

    col_a = at(core * half + x * eighth, eighth)
    col_b = at(core * half + quarter + x * eighth, eighth)
    for s in range(lines - 1):
        arrive("3", s)
    for n, col in enumerate((col_a, col_b)):
        total = own[n]
        for s in range(lines - 1):
            total = total + r3[s, :, n * eighth : (n + 1) * eighth].astype(f32)
        outer_grad = total * 0.25
        momentum = outer_beta * mom[:, col] + outer_grad
        fresh[:, col] = momentum.astype(fresh.dtype)
        params = glob[:, col] - outer_rate * (outer_grad + outer_beta * momentum)
        weights[z, y, :, col] = params.astype(weights.dtype)

    def swap(kind, step, ref, peer):
        send(kind, step, ref, ref, peer)

    def from_line(step):
        return lax.rem(z + lines - step, lines)

    for t in range(1, lines):
        peer = over_z(lax.rem(z + t, lines))
        swap("g3a", t, weights.at[z, y, :, col_a], peer)
        swap("g3b", t, weights.at[z, y, :, col_b], peer)

    def landed(kind, step, ref):
        copy = copies[kind, step]
        copy.wait_recv()

    def gather_third(t):
        g = from_line(t)
        if t:
            landed("g3a", t, None)
        swap("g2a", t, weights.at[g, y, :, col_a], over_y)
        if t:
            landed("g3b", t, None)
        swap("g2b", t, weights.at[g, y, :, col_b], over_x)
        if not t:
            swap("ma", 0, fresh.at[:, col_a], over_x)
            swap("mb", 0, fresh.at[:, col_b], over_x)

    def gather_second(t):
        g = from_line(t)
        arrive("g2a", t)
        swap("g1a", t, weights.at[g, :, :, col_a], over_x)
        arrive("g2b", t)
        swap("g1b", t, weights.at[g, y, :, at(core * half + quarter, quarter)], over_y)

    def gather_first(t):
        g = from_line(t)
        arrive("g1a", t)
        arrive("g1b", t)
        swap("gc", t, weights.at[g, :, :, at(core * half, half)], over_core)

    for tick in range(lines + 2):
        if 0 <= tick - 2:
            gather_first(tick - 2)
        if 0 <= tick - 1 < lines:
            gather_second(tick - 1)
        if tick < lines:
            gather_third(tick)
    arrive("ma", 0)
    arrive("mb", 0)
    swap("mc", 0, fresh.at[:, at(core * half, half)], over_core)
    for t in range(lines):
        arrive("gc", t)
    arrive("mc", 0)
    for copy in copies.values():
        copy.wait_send()


def outer_step(part, glob, mom):
    lines, pair, rows, cols = part.shape
    low = jnp.bfloat16
    half, quarter, eighth = cols // 2, cols // 4, cols // 8
    count = lines * 5 + lines - 1 + 2 * (lines - 1) + lines * 5 + 3
    vmem = pl.BlockSpec(memory_space=pltpu.VMEM)
    return pl.pallas_call(
        outer_kernel,
        out_shape=(
            jax.ShapeDtypeStruct(part.shape, low),
            jax.ShapeDtypeStruct((rows, cols), low),
        ),
        in_specs=[vmem] * 3,
        out_specs=(vmem, vmem),
        scratch_shapes=[
            pltpu.VMEM((lines, pair, rows, half), low),
            pltpu.VMEM((lines, pair, rows, eighth), low),
            pltpu.VMEM((lines, rows, quarter), low),
            pltpu.VMEM((lines, rows, eighth), low),
            pltpu.VMEM((lines, rows, eighth), low),
            pltpu.VMEM((lines - 1, rows, quarter), low),
            pltpu.VMEM((lines - 1, rows, quarter), low),
            pltpu.SemaphoreType.DMA((count,)),
            pltpu.SemaphoreType.DMA((count,)),
        ],
        compiler_params=pltpu.CompilerParams(
            collective_id=0, has_side_effects=True, vmem_limit_bytes=60 * 2**20
        ),
    )(part, glob, mom)


def body(
    layer_inputs,
    queries,
    saved_keys,
    saved_values,
    out_grad,
    global_params,
    replica_params,
    outer_momentum,
    next_inputs,
):
    key_grad = attention_keys(queries, saved_keys, saved_values, out_grad)
    shards = lax.axis_size("fsdp")
    mine = lax.axis_index("fsdp")
    rows, cols = global_params.shape
    drift = global_params - replica_params[0]
    partial = inner_rate * lax.dot_general(
        layer_inputs, key_grad, (((0,), (0,)), ((), ())), preferred_element_type=jnp.float32
    )
    partial = partial.astype(jnp.bfloat16)
    block = lax.dynamic_slice_in_dim(partial, mine * rows, rows, 0)
    block = (block.astype(jnp.float32) + drift).astype(jnp.bfloat16)
    partial = lax.dynamic_update_slice_in_dim(partial, block, mine * rows, 0)
    weights, momentum = outer_step(
        partial.reshape(shards // 2, 2, rows, cols), global_params, outer_momentum
    )
    weights = weights.reshape(shards * rows, cols)
    projected = jnp.dot(next_inputs, weights, preferred_element_type=jnp.float32)
    own = lax.dynamic_slice_in_dim(weights, mine * rows, rows, 0)
    return (
        own.astype(jnp.float32),
        momentum.astype(jnp.float32),
        projected.astype(jnp.bfloat16),
    )


def solution(mesh):
    return jax.shard_map(
        body,
        mesh=mesh,
        in_specs=(
            P(("rep", "fsdp"), None),
            P(("rep", "fsdp"), None),
            P(("rep", "fsdp"), None),
            P(("rep", "fsdp"), None),
            P(("rep", "fsdp"), None),
            P("fsdp", None),
            P("rep", "fsdp", None),
            P("fsdp", None),
            P(("rep", "fsdp"), None),
        ),
        out_specs=(P("fsdp", None), P("fsdp", None), P(("rep", "fsdp"), None)),
        check_vma=False,
    )
```

```python
import functools

import jax
import jax.numpy as jnp
import numpy as np
from jax import lax
from jax.experimental import pallas as pl
from jax.experimental.pallas import tpu as pltpu
from jax.sharding import PartitionSpec as P

QH = 16
KVH = 8
HD = 128


score_scale = 1.0 / 12.0
soft_cap = 50.0
rope_base = 10000.0
inner_rate = 0.02
outer_rate = 0.7
outer_beta = 0.9

MESH = pl.DeviceIdType.MESH


def attention_kernel(q_ref, k_ref, v_ref, g_ref, cos_ref, sin_ref, out_ref):
    length = k_ref.shape[0]
    f32 = jnp.float32
    keys, values = k_ref[...], v_ref[...]
    row = lax.broadcasted_iota(jnp.int32, (length, length), 0)
    column = lax.broadcasted_iota(jnp.int32, (length, length), 1)
    causal = row >= column
    across = (((1,), (1,)), ((), ()))
    rotated = jnp.zeros((length, HD), f32)
    for j in range(QH // KVH):
        cols = slice(j * HD, (j + 1) * HD)
        query = q_ref[:, cols]
        logits = lax.dot_general(query, keys, across, preferred_element_type=f32)
        capped = jnp.tanh(logits * (score_scale / soft_cap))
        unnormed = jnp.where(causal, jnp.exp(soft_cap * capped), 0.0)
        probs = unnormed / jnp.sum(unnormed, axis=-1, keepdims=True)
        dprobs = lax.dot_general(g_ref[:, cols], values, across, preferred_element_type=f32)
        center = jnp.sum(probs * dprobs, axis=-1, keepdims=True)
        dlogits = probs * (dprobs - center) * (1.0 - capped * capped) * score_scale
        rotated += lax.dot_general(
            dlogits.astype(jnp.bfloat16),
            query,
            (((0,), (0,)), ((), ())),
            preferred_element_type=f32,
        )
    swapped = jnp.concatenate([rotated[:, HD // 2 :], rotated[:, : HD // 2]], axis=-1)
    out_ref[...] = (rotated * cos_ref[...] + swapped * sin_ref[...]).astype(out_ref.dtype)


def attention_keys(query_rows, key_rows, value_rows, grad_rows):
    length = query_rows.shape[0]
    group = QH // KVH
    half = HD // 2
    freqs = np.float32(rope_base) ** (-np.arange(half, dtype=np.float32) / np.float32(half))
    angles = (np.arange(length, dtype=np.float32)[:, None] * freqs[None, :]).astype(np.float64)
    cosine = np.concatenate([np.cos(angles)] * 2, axis=1).astype(np.float32)
    sine = np.concatenate([np.sin(angles), -np.sin(angles)], axis=1).astype(np.float32)
    wide = pl.BlockSpec((length, group * HD), lambda h: (0, h))
    narrow = pl.BlockSpec((length, HD), lambda h: (0, h))
    table = pl.BlockSpec((length, HD), lambda h: (0, 0))
    return pl.pallas_call(
        attention_kernel,
        grid=(KVH,),
        out_shape=jax.ShapeDtypeStruct((length, KVH * HD), jnp.bfloat16),
        in_specs=[wide, narrow, narrow, wide, table, table],
        out_specs=narrow,
    )(query_rows, key_rows, value_rows, grad_rows, jnp.asarray(cosine), jnp.asarray(sine))


def outer_kernel(inside, *refs):
    if inside:
        (layer, keyg, drift, nxt_in, glob_in, mom_in, fresh, own_out, proj) = refs[:9]
        (part, weights, nxt, total_ref, load_sem, *rest) = refs[9:]
    else:
        (part, glob_in, mom_in, fresh, weights, load_sem, *rest) = refs
    glob, mom, rc, r1a, r1b, r2a, r2b, s3, r3, send_sem, recv_sem = rest
    lines = part.shape[0]
    rows, cols = glob.shape
    half, quarter, eighth = cols // 2, cols // 4, cols // 8
    rep, fsdp = lax.axis_index("rep"), lax.axis_index("fsdp")
    core, x = lax.rem(rep, 2), rep // 2
    y, z = lax.rem(fsdp, 2), fsdp // 2
    over_core = {"rep": rep + 1 - 2 * core}
    over_x = {"rep": rep + 2 - 4 * x}
    over_y = {"fsdp": fsdp + 1 - 2 * y}
    every = slice(None)

    def over_z(line):
        return {"fsdp": line * 2 + y}

    def at(start, size):
        return pl.ds(pl.multiple_of(start, size), size)

    def pair(ref, g, col=every):
        return ref.at[g, :, col] if inside else ref.at[g, :, :, col]

    def block(ref, g, yy, col=every):
        if inside:
            return ref.at[g, at(yy * rows, rows), col]
        return ref.at[g, yy, :, col]

    loads = [
        pltpu.make_async_copy(src, dst, load_sem.at[n])
        for n, (src, dst) in enumerate(
            [(glob_in, glob), (mom_in, mom)] + ([(nxt_in, nxt)] if inside else [])
        )
    ]
    for load in loads:
        load.start()

    f32 = jnp.float32
    peers = [over_core, over_x, over_y] + [
        over_z(lax.rem(z + t, lines)) for t in range(1, lines)
    ]
    barrier = pltpu.get_barrier_semaphore()
    for peer in peers:
        pl.semaphore_signal(barrier, inc=1, device_id=peer, device_id_type=MESH)
    pl.semaphore_wait(barrier, len(peers))

    copies = {}

    def send(kind, step, src, dst, peer):
        slot = len(copies)
        copy = pltpu.make_async_remote_copy(
            src_ref=src,
            dst_ref=dst,
            send_sem=send_sem.at[slot],
            recv_sem=recv_sem.at[slot],
            device_id=peer,
            device_id_type=MESH,
        )
        copy.start()
        copies[kind, step] = copy

    def arrive(kind, step):
        copies[kind, step].wait_recv()

    def line_of(step):
        return lax.rem(z + 1 + step, lines)

    def multiply(s):
        g = line_of(s)
        if inside:
            width = 2 * rows
            tile = 128

            def one(n, carry):
                left = layer[:, at(g * width + n * tile, tile)]
                result = lax.dot_general(
                    left, keyg[...], (((0,), (0,)), ((), ())), preferred_element_type=f32
                )
                part[g, at(n * tile, tile), :] = (result * inner_rate).astype(part.dtype)
                return carry

            lax.fori_loop(0, width // tile, one, 0)
            if s == lines - 1:
                mine = block(part, g, y)
                mine[...] = (mine[...].astype(f32) + (glob[...] - drift[...])).astype(part.dtype)
        theirs = at((1 - core) * half, half)
        send("c", s, pair(part, g, theirs), pair(rc, g), over_core)

    def sum_core(s):
        g = line_of(s)
        arrive("c", s)
        for yy in range(2):
            mine = block(part, g, yy, at(core * half, half))[...]
            sums = block(rc, g, yy)
            sums[...] = (sums[...].astype(f32) + mine.astype(f32)).astype(rc.dtype)
        send("1a", s, pair(rc, g, at((1 - x) * eighth, eighth)), pair(r1a, g), over_x)
        send("1b", s, block(rc, g, 1 - y, slice(quarter, half)), r1b.at[g], over_y)

    def sum_first(s):
        g = line_of(s)
        arrive("1a", s)
        for yy in range(2):
            mine = block(rc, g, yy, at(x * eighth, eighth))[...]
            sums = block(r1a, g, yy)
            sums[...] = (sums[...].astype(f32) + mine.astype(f32)).astype(rc.dtype)
        send("2a", s, block(r1a, g, 1 - y), r2a.at[g], over_y)
        arrive("1b", s)
        mine = block(rc, g, y, slice(quarter, half))[...]
        r1b[g] = (r1b[g].astype(f32) + mine.astype(f32)).astype(rc.dtype)
        send("2b", s, r1b.at[g, :, at((1 - x) * eighth, eighth)], r2b.at[g], over_x)

    def sum_second(s):
        g = line_of(s)
        arrive("2a", s)
        sum_a = r2a[g].astype(f32) + block(r1a, g, y)[...].astype(f32)
        arrive("2b", s)
        sum_b = r2b[g].astype(f32) + r1b[g, :, at(x * eighth, eighth)].astype(f32)
        if s == lines - 1:
            return sum_a, sum_b
        s3[s, :, :eighth] = sum_a.astype(s3.dtype)
        s3[s, :, eighth:] = sum_b.astype(s3.dtype)
        send("3", s, s3.at[s], r3.at[s], over_z(g))

    for load in loads[:2]:
        load.wait()
    for s in range(lines):
        multiply(s)
        if s >= 1:
            sum_core(s - 1)
        if s >= 2:
            sum_first(s - 2)
        if s >= 3:
            sum_second(s - 3)
    sum_core(lines - 1)
    for s in range(max(lines - 2, 0), lines):
        sum_first(s)
    for s in range(max(lines - 3, 0), lines):
        own = sum_second(s)

    col_a = at(core * half + x * eighth, eighth)
    col_b = at(core * half + quarter + x * eighth, eighth)
    for s in range(lines - 1):
        arrive("3", s)
    for n, col in enumerate((col_a, col_b)):
        total = own[n]
        for s in range(lines - 1):
            total = total + r3[s, :, n * eighth : (n + 1) * eighth].astype(f32)
        outer_grad = total * 0.25
        momentum = outer_beta * mom[:, col] + outer_grad
        fresh[:, col] = momentum.astype(fresh.dtype)
        params = glob[:, col] - outer_rate * (outer_grad + outer_beta * momentum)
        block(weights, z, y, col)[...] = params.astype(weights.dtype)

    def swap(kind, step, ref, peer):
        send(kind, step, ref, ref, peer)

    def from_line(step):
        return lax.rem(z + lines - step, lines)

    for t in range(1, lines):
        peer = over_z(lax.rem(z + t, lines))
        swap("g3a", t, block(weights, z, y, col_a), peer)
        swap("g3b", t, block(weights, z, y, col_b), peer)

    def gather_third(t):
        g = from_line(t)
        if t:
            arrive("g3a", t)
        swap("g2a", t, block(weights, g, y, col_a), over_y)
        if t:
            arrive("g3b", t)
        swap("g2b", t, block(weights, g, y, col_b), over_x)
        if not t:
            swap("ma", 0, fresh.at[:, col_a], over_x)
            swap("mb", 0, fresh.at[:, col_b], over_x)

    def gather_second(t):
        g = from_line(t)
        arrive("g2a", t)
        swap("g1a", t, pair(weights, g, col_a), over_x)
        arrive("g2b", t)
        swap("g1b", t, block(weights, g, y, at(core * half + quarter, quarter)), over_y)

    def gather_first(t):
        g = from_line(t)
        arrive("g1a", t)
        arrive("g1b", t)
        swap("gc", t, pair(weights, g, at(core * half, half)), over_core)

    def project(t):
        g = from_line(t)
        arrive("gc", t)
        if not inside:
            return
        left = nxt[:, at(g * 2 * rows, 2 * rows)]
        for n in range(2):
            col = slice(n * half, (n + 1) * half)
            result = jnp.dot(left, weights[g, :, col], preferred_element_type=f32)
            total_ref[:, col] = result if not t else total_ref[:, col] + result

    if inside:
        loads[2].wait()
    for tick in range(lines + 3):
        if tick < lines:
            gather_third(tick)
        if 0 <= tick - 1 < lines:
            gather_second(tick - 1)
        if 0 <= tick - 2 < lines:
            gather_first(tick - 2)
        if tick == 2:
            arrive("ma", 0)
            arrive("mb", 0)
            swap("mc", 0, fresh.at[:, at(core * half, half)], over_core)
        if 0 <= tick - 3:
            project(tick - 3)
    arrive("mc", 0)
    if inside:
        own_out[...] = block(weights, z, y)[...]
        proj[...] = total_ref[...].astype(proj.dtype)
    for copy in copies.values():
        copy.wait_send()


def outer_step(layer_inputs, key_grad, next_inputs, global_params, own_params, momentum):
    tokens, depth = layer_inputs.shape
    rows, cols = global_params.shape
    lines = depth // (2 * rows)
    inside = (2 * rows) % 128 == 0
    low, f32 = jnp.bfloat16, jnp.float32
    half, quarter, eighth = cols // 2, cols // 4, cols // 8
    count = lines * 5 + lines - 1 + 2 * (lines - 1) + lines * 5 + 3
    both = (lines, 2 * rows) if inside else (lines, 2, rows)
    vmem = pl.BlockSpec(memory_space=pltpu.VMEM)
    hbm = pl.BlockSpec(memory_space=pl.ANY)
    shared = [
        pltpu.SemaphoreType.DMA((3,)),
        pltpu.VMEM((rows, cols), f32),
        pltpu.VMEM((rows, cols), f32),
        pltpu.VMEM((*both, half), low),
        pltpu.VMEM((*both, eighth), low),
        pltpu.VMEM((lines, rows, quarter), low),
        pltpu.VMEM((lines, rows, eighth), low),
        pltpu.VMEM((lines, rows, eighth), low),
        pltpu.VMEM((lines - 1, rows, quarter), low),
        pltpu.VMEM((lines - 1, rows, quarter), low),
        pltpu.SemaphoreType.DMA((count,)),
        pltpu.SemaphoreType.DMA((count,)),
    ]
    params = pltpu.CompilerParams(
        collective_id=0, has_side_effects=True, vmem_limit_bytes=62 * 2**20
    )
    block = jax.ShapeDtypeStruct((rows, cols), low)
    kernel = functools.partial(outer_kernel, inside)
    if inside:
        fresh, own, projected = pl.pallas_call(
            kernel,
            out_shape=(block, block, jax.ShapeDtypeStruct((tokens, cols), low)),
            in_specs=[vmem] * 3 + [hbm] * 3,
            out_specs=(vmem,) * 3,
            scratch_shapes=[
                pltpu.VMEM((*both, cols), low),
                pltpu.VMEM((*both, cols), low),
                pltpu.VMEM((tokens, depth), low),
                pltpu.VMEM((tokens, cols), f32),
                *shared,
            ],
            compiler_params=params,
        )(layer_inputs, key_grad, own_params, next_inputs, global_params, momentum)
        return own.astype(f32), fresh.astype(f32), projected
    start = lax.axis_index("fsdp") * rows
    partial = inner_rate * lax.dot_general(
        layer_inputs, key_grad, (((0,), (0,)), ((), ())), preferred_element_type=f32
    )
    mine = lax.dynamic_slice_in_dim(partial, start, rows, 0) + (global_params - own_params)
    partial = lax.dynamic_update_slice_in_dim(partial, mine, start, 0).astype(low)
    fresh, weights = pl.pallas_call(
        kernel,
        out_shape=(block, jax.ShapeDtypeStruct((*both, cols), low)),
        in_specs=[vmem] + [hbm] * 2,
        out_specs=(vmem,) * 2,
        scratch_shapes=shared,
        compiler_params=params,
    )(partial.reshape(*both, cols), global_params, momentum)
    weights = weights.reshape(depth, cols)
    projected = jnp.dot(next_inputs, weights, preferred_element_type=f32)
    own = lax.dynamic_slice_in_dim(weights, start, rows, 0)
    return own.astype(f32), fresh.astype(f32), projected.astype(low)


def body(
    layer_inputs,
    queries,
    saved_keys,
    saved_values,
    out_grad,
    global_params,
    replica_params,
    outer_momentum,
    next_inputs,
):
    key_grad = attention_keys(queries, saved_keys, saved_values, out_grad)
    return outer_step(
        layer_inputs, key_grad, next_inputs, global_params, replica_params[0], outer_momentum
    )


def solution(mesh):
    return jax.shard_map(
        body,
        mesh=mesh,
        in_specs=(
            P(("rep", "fsdp"), None),
            P(("rep", "fsdp"), None),
            P(("rep", "fsdp"), None),
            P(("rep", "fsdp"), None),
            P(("rep", "fsdp"), None),
            P("fsdp", None),
            P("rep", "fsdp", None),
            P("fsdp", None),
            P(("rep", "fsdp"), None),
        ),
        out_specs=(P("fsdp", None), P("fsdp", None), P(("rep", "fsdp"), None)),
        check_vma=False,
    )
```

```python
import functools

import jax
import jax.numpy as jnp
import numpy as np
from jax import lax
from jax.experimental import pallas as pl
from jax.experimental.pallas import tpu as pltpu
from jax.sharding import PartitionSpec as P

QH = 16
KVH = 8
HD = 128


score_scale = 1.0 / 12.0
soft_cap = 50.0
rope_base = 10000.0
inner_rate = 0.02
outer_rate = 0.7
outer_beta = 0.9

MESH = pl.DeviceIdType.MESH


def attention_kernel(q_ref, k_ref, v_ref, g_ref, cos_ref, sin_ref, out_ref):
    length = k_ref.shape[0]
    f32 = jnp.float32
    keys, values = k_ref[...], v_ref[...]
    row = lax.broadcasted_iota(jnp.int32, (length, length), 0)
    column = lax.broadcasted_iota(jnp.int32, (length, length), 1)
    causal = row >= column
    across = (((1,), (1,)), ((), ()))
    rotated = jnp.zeros((length, HD), f32)
    for j in range(QH // KVH):
        cols = slice(j * HD, (j + 1) * HD)
        query = q_ref[:, cols]
        logits = lax.dot_general(query, keys, across, preferred_element_type=f32)
        capped = jnp.tanh(logits * (score_scale / soft_cap))
        unnormed = jnp.where(causal, jnp.exp(soft_cap * capped), 0.0)
        probs = unnormed / jnp.sum(unnormed, axis=-1, keepdims=True)
        dprobs = lax.dot_general(g_ref[:, cols], values, across, preferred_element_type=f32)
        center = jnp.sum(probs * dprobs, axis=-1, keepdims=True)
        dlogits = probs * (dprobs - center) * (1.0 - capped * capped) * score_scale
        rotated += lax.dot_general(
            dlogits.astype(jnp.bfloat16),
            query,
            (((0,), (0,)), ((), ())),
            preferred_element_type=f32,
        )
    swapped = jnp.concatenate([rotated[:, HD // 2 :], rotated[:, : HD // 2]], axis=-1)
    out_ref[...] = (rotated * cos_ref[...] + swapped * sin_ref[...]).astype(out_ref.dtype)


def attention_keys(query_rows, key_rows, value_rows, grad_rows):
    length = query_rows.shape[0]
    group = QH // KVH
    half = HD // 2
    freqs = np.float32(rope_base) ** (-np.arange(half, dtype=np.float32) / np.float32(half))
    angles = (np.arange(length, dtype=np.float32)[:, None] * freqs[None, :]).astype(np.float64)
    cosine = np.concatenate([np.cos(angles)] * 2, axis=1).astype(np.float32)
    sine = np.concatenate([np.sin(angles), -np.sin(angles)], axis=1).astype(np.float32)
    wide = pl.BlockSpec((length, group * HD), lambda h: (0, h))
    narrow = pl.BlockSpec((length, HD), lambda h: (0, h))
    table = pl.BlockSpec((length, HD), lambda h: (0, 0))
    return pl.pallas_call(
        attention_kernel,
        grid=(KVH,),
        out_shape=jax.ShapeDtypeStruct((length, KVH * HD), jnp.bfloat16),
        in_specs=[wide, narrow, narrow, wide, table, table],
        out_specs=narrow,
    )(query_rows, key_rows, value_rows, grad_rows, jnp.asarray(cosine), jnp.asarray(sine))


def outer_kernel(inside, *refs):
    if inside:
        (keyg, layer_in, drift_in, nxt_in, glob_in, mom_in, fresh, own_out, proj) = refs[:9]
        (part, weights, layer, drift, nxt, total_ref, load_sem, *rest) = refs[9:]
    else:
        (part, glob_in, mom_in, fresh, weights, load_sem, *rest) = refs
    glob, mom, rc, r1a, r1b, r2a, r2b, s3, r3, send_sem, recv_sem = rest
    lines = part.shape[0]
    rows, cols = glob.shape
    half, quarter, eighth = cols // 2, cols // 4, cols // 8
    rep, fsdp = lax.axis_index("rep"), lax.axis_index("fsdp")
    core, x = lax.rem(rep, 2), rep // 2
    y, z = lax.rem(fsdp, 2), fsdp // 2
    over_core = {"rep": rep + 1 - 2 * core}
    over_x = {"rep": rep + 2 - 4 * x}
    over_y = {"fsdp": fsdp + 1 - 2 * y}
    every = slice(None)

    def over_z(line):
        return {"fsdp": line * 2 + y}

    def at(start, size):
        return pl.ds(pl.multiple_of(start, size), size)

    def pair(ref, g, col=every):
        return ref.at[g, :, col] if inside else ref.at[g, :, :, col]

    def block(ref, g, yy, col=every):
        if inside:
            return ref.at[g, at(yy * rows, rows), col]
        return ref.at[g, yy, :, col]

    def line_of(step):
        return lax.rem(z + 1 + step, lines)

    moves = []
    if inside:
        for s in range(lines):
            cols_of = at(line_of(s) * 2 * rows, 2 * rows)
            moves.append((layer_in.at[:, cols_of], layer.at[:, cols_of]))
        moves.append((drift_in, drift))
    moves.append((glob_in, glob))
    moves.append((mom_in, mom))
    if inside:
        moves.append((nxt_in, nxt))
    loads = [
        pltpu.make_async_copy(src, dst, load_sem.at[n]) for n, (src, dst) in enumerate(moves)
    ]
    for load in loads:
        load.start()

    f32 = jnp.float32
    peers = [over_core, over_x, over_y] + [
        over_z(lax.rem(z + t, lines)) for t in range(1, lines)
    ]
    barrier = pltpu.get_barrier_semaphore()
    for peer in peers:
        pl.semaphore_signal(barrier, inc=1, device_id=peer, device_id_type=MESH)
    pl.semaphore_wait(barrier, len(peers))

    copies = {}

    def send(kind, step, src, dst, peer):
        slot = len(copies)
        copy = pltpu.make_async_remote_copy(
            src_ref=src,
            dst_ref=dst,
            send_sem=send_sem.at[slot],
            recv_sem=recv_sem.at[slot],
            device_id=peer,
            device_id_type=MESH,
        )
        copy.start()
        copies[kind, step] = copy

    def arrive(kind, step):
        copies[kind, step].wait_recv()

    def multiply(s):
        g = line_of(s)
        theirs, own_half = at((1 - core) * half, half), at(core * half, half)
        if inside:
            width = 2 * rows
            tile = 128
            loads[s].wait()
            if s == lines - 1:
                for load in loads[lines : lines + 2]:
                    load.wait()

            def product(col):
                def one(n, carry):
                    left = layer[:, at(g * width + n * tile, tile)]
                    result = lax.dot_general(
                        left,
                        keyg[:, col],
                        (((0,), (0,)), ((), ())),
                        preferred_element_type=f32,
                    )
                    part[g, at(n * tile, tile), col] = (result * inner_rate).astype(part.dtype)
                    return carry

                lax.fori_loop(0, width // tile, one, 0)
                if s == lines - 1:
                    mine = block(part, g, y, col)
                    moved = glob[:, col] - drift[:, col]
                    mine[...] = (mine[...].astype(f32) + moved).astype(part.dtype)

            product(theirs)
        send("c", s, pair(part, g, theirs), pair(rc, g), over_core)
        if inside:
            product(own_half)

    def sum_core(s):
        g = line_of(s)
        arrive("c", s)
        for yy in range(2):
            mine = block(part, g, yy, at(core * half, half))[...]
            sums = block(rc, g, yy)
            sums[...] = (sums[...].astype(f32) + mine.astype(f32)).astype(rc.dtype)
        send("1a", s, pair(rc, g, at((1 - x) * eighth, eighth)), pair(r1a, g), over_x)
        send("1b", s, block(rc, g, 1 - y, slice(quarter, half)), r1b.at[g], over_y)

    def sum_first(s):
        g = line_of(s)
        arrive("1a", s)
        for yy in range(2):
            mine = block(rc, g, yy, at(x * eighth, eighth))[...]
            sums = block(r1a, g, yy)
            sums[...] = (sums[...].astype(f32) + mine.astype(f32)).astype(rc.dtype)
        send("2a", s, block(r1a, g, 1 - y), r2a.at[g], over_y)
        arrive("1b", s)
        mine = block(rc, g, y, slice(quarter, half))[...]
        r1b[g] = (r1b[g].astype(f32) + mine.astype(f32)).astype(rc.dtype)
        send("2b", s, r1b.at[g, :, at((1 - x) * eighth, eighth)], r2b.at[g], over_x)

    def sum_second(s):
        g = line_of(s)
        arrive("2a", s)
        sum_a = r2a[g].astype(f32) + block(r1a, g, y)[...].astype(f32)
        arrive("2b", s)
        sum_b = r2b[g].astype(f32) + r1b[g, :, at(x * eighth, eighth)].astype(f32)
        if s == lines - 1:
            return sum_a, sum_b
        s3[s, :, :eighth] = sum_a.astype(s3.dtype)
        s3[s, :, eighth:] = sum_b.astype(s3.dtype)
        send("3", s, s3.at[s], r3.at[s], over_z(g))

    multiply(0)
    sum_core(0)
    for s in range(1, lines):
        multiply(s)
        sum_core(s)
        sum_first(s - 1)
        if s >= 2:
            sum_second(s - 2)
    sum_first(lines - 1)
    if lines > 1:
        sum_second(lines - 2)
    own = sum_second(lines - 1)

    for load in loads[lines + 2 :] if inside else loads:
        load.wait()
    col_a = at(core * half + x * eighth, eighth)
    col_b = at(core * half + quarter + x * eighth, eighth)
    for s in range(lines - 1):
        arrive("3", s)
    for n, col in enumerate((col_a, col_b)):
        total = own[n]
        for s in range(lines - 1):
            total = total + r3[s, :, n * eighth : (n + 1) * eighth].astype(f32)
        outer_grad = total * 0.25
        momentum = outer_beta * mom[:, col] + outer_grad
        fresh[:, col] = momentum.astype(fresh.dtype)
        params = glob[:, col] - outer_rate * (outer_grad + outer_beta * momentum)
        block(weights, z, y, col)[...] = params.astype(weights.dtype)

    def swap(kind, step, ref, peer):
        send(kind, step, ref, ref, peer)

    def from_line(step):
        return lax.rem(z + lines - step, lines)

    for t in range(1, lines):
        peer = over_z(lax.rem(z + t, lines))
        swap("g3a", t, block(weights, z, y, col_a), peer)
        swap("g3b", t, block(weights, z, y, col_b), peer)

    def gather_third(t):
        g = from_line(t)
        if t:
            arrive("g3a", t)
        swap("g2a", t, block(weights, g, y, col_a), over_y)
        if t:
            arrive("g3b", t)
        swap("g2b", t, block(weights, g, y, col_b), over_x)

    def gather_second(t):
        g = from_line(t)
        arrive("g2a", t)
        swap("g1a", t, pair(weights, g, col_a), over_x)
        arrive("g2b", t)
        swap("g1b", t, block(weights, g, y, at(core * half + quarter, quarter)), over_y)

    def gather_first(t):
        g = from_line(t)
        arrive("g1a", t)
        arrive("g1b", t)
        swap("gc", t, pair(weights, g, at(core * half, half)), over_core)

    def project(t):
        g = from_line(t)
        arrive("gc", t)
        if not inside:
            return
        left = nxt[:, at(g * 2 * rows, 2 * rows)]
        for n in range(2):
            col = slice(n * half, (n + 1) * half)
            result = jnp.dot(left, weights[g, :, col], preferred_element_type=f32)
            total_ref[:, col] = result if not t else total_ref[:, col] + result

    gather_third(0)
    gather_second(0)
    if lines > 1:
        gather_third(1)
    swap("ma", 0, fresh.at[:, col_a], over_x)
    swap("mb", 0, fresh.at[:, col_b], over_x)
    for t in range(1, lines):
        if t == 1:
            gather_first(0)
        gather_second(t)
        if t + 1 < lines:
            gather_third(t + 1)
        if t > 1:
            gather_first(t - 1)
            project(t - 2)
        else:
            arrive("ma", 0)
            arrive("mb", 0)
            swap("mc", 0, fresh.at[:, at(core * half, half)], over_core)
    gather_first(lines - 1)
    if lines > 1:
        project(lines - 2)
    arrive("mc", 0)
    project(lines - 1)
    if inside:
        own_out[...] = block(weights, z, y)[...]
        proj[...] = total_ref[...].astype(proj.dtype)
    for copy in copies.values():
        copy.wait_send()


def outer_step(layer_inputs, key_grad, next_inputs, global_params, own_params, momentum):
    tokens, depth = layer_inputs.shape
    rows, cols = global_params.shape
    lines = depth // (2 * rows)
    inside = (2 * rows) % 128 == 0
    low, f32 = jnp.bfloat16, jnp.float32
    half, quarter, eighth = cols // 2, cols // 4, cols // 8
    count = lines * 5 + lines - 1 + 2 * (lines - 1) + lines * 5 + 3
    both = (lines, 2 * rows) if inside else (lines, 2, rows)
    vmem = pl.BlockSpec(memory_space=pltpu.VMEM)
    hbm = pl.BlockSpec(memory_space=pl.ANY)
    shared = [
        pltpu.SemaphoreType.DMA((lines + 4,)),
        pltpu.VMEM((rows, cols), f32),
        pltpu.VMEM((rows, cols), f32),
        pltpu.VMEM((*both, half), low),
        pltpu.VMEM((*both, eighth), low),
        pltpu.VMEM((lines, rows, quarter), low),
        pltpu.VMEM((lines, rows, eighth), low),
        pltpu.VMEM((lines, rows, eighth), low),
        pltpu.VMEM((lines - 1, rows, quarter), low),
        pltpu.VMEM((lines - 1, rows, quarter), low),
        pltpu.SemaphoreType.DMA((count,)),
        pltpu.SemaphoreType.DMA((count,)),
    ]
    params = pltpu.CompilerParams(
        collective_id=0, has_side_effects=True, vmem_limit_bytes=62 * 2**20
    )
    block = jax.ShapeDtypeStruct((rows, cols), low)
    kernel = functools.partial(outer_kernel, inside)
    if inside:
        fresh, own, projected = pl.pallas_call(
            kernel,
            out_shape=(block, block, jax.ShapeDtypeStruct((tokens, cols), low)),
            in_specs=[vmem] + [hbm] * 5,
            out_specs=(vmem,) * 3,
            scratch_shapes=[
                pltpu.VMEM((*both, cols), low),
                pltpu.VMEM((*both, cols), low),
                pltpu.VMEM((tokens, depth), low),
                pltpu.VMEM((rows, cols), f32),
                pltpu.VMEM((tokens, depth), low),
                pltpu.VMEM((tokens, cols), f32),
                *shared,
            ],
            compiler_params=params,
        )(key_grad, layer_inputs, own_params, next_inputs, global_params, momentum)
        return own.astype(f32), fresh.astype(f32), projected
    start = lax.axis_index("fsdp") * rows
    partial = inner_rate * lax.dot_general(
        layer_inputs, key_grad, (((0,), (0,)), ((), ())), preferred_element_type=f32
    )
    mine = lax.dynamic_slice_in_dim(partial, start, rows, 0) + (global_params - own_params)
    partial = lax.dynamic_update_slice_in_dim(partial, mine, start, 0).astype(low)
    fresh, weights = pl.pallas_call(
        kernel,
        out_shape=(block, jax.ShapeDtypeStruct((*both, cols), low)),
        in_specs=[vmem] + [hbm] * 2,
        out_specs=(vmem,) * 2,
        scratch_shapes=shared,
        compiler_params=params,
    )(partial.reshape(*both, cols), global_params, momentum)
    weights = weights.reshape(depth, cols)
    projected = jnp.dot(next_inputs, weights, preferred_element_type=f32)
    own = lax.dynamic_slice_in_dim(weights, start, rows, 0)
    return own.astype(f32), fresh.astype(f32), projected.astype(low)


def body(
    layer_inputs,
    queries,
    saved_keys,
    saved_values,
    out_grad,
    global_params,
    replica_params,
    outer_momentum,
    next_inputs,
):
    key_grad = attention_keys(queries, saved_keys, saved_values, out_grad)
    return outer_step(
        layer_inputs, key_grad, next_inputs, global_params, replica_params[0], outer_momentum
    )


def solution(mesh):
    return jax.shard_map(
        body,
        mesh=mesh,
        in_specs=(
            P(("rep", "fsdp"), None),
            P(("rep", "fsdp"), None),
            P(("rep", "fsdp"), None),
            P(("rep", "fsdp"), None),
            P(("rep", "fsdp"), None),
            P("fsdp", None),
            P("rep", "fsdp", None),
            P("fsdp", None),
            P(("rep", "fsdp"), None),
        ),
        out_specs=(P("fsdp", None), P("fsdp", None), P(("rep", "fsdp"), None)),
        check_vma=False,
    )
```
